32 devices in a mesh: dp: 4 (over x, y), tp: 8 (over z, core).
Axes of the slice: x: 2, y: 2, z: 4, core: 2. Of those that a mesh axis runs over, the one named last changes fastest.
Arguments:
- x: bfloat16 [8192, 4096], P('dp'), parts along dimension 0
- dy: bfloat16 [8192, 4096], P('dp'), parts along dimension 0
- gate: bfloat16 [8192, 16384], P('dp', 'tp'), parts along dimension 0
- up: bfloat16 [8192, 16384], P('dp', 'tp'), parts along dimension 0
- w_gate: bfloat16 [4096, 16384], P(None, 'tp')
- w_up: bfloat16 [4096, 16384], P(None, 'tp')
- w_down: bfloat16 [16384, 4096], P('tp')
Outputs:
- output 1: bfloat16 [8192, 4096], P('dp'), parts along dimension 0
- output 2: bfloat16 [16384, 16384], P('dp', 'tp'), parts along dimension 0
- output 3: bfloat16 [16384, 16384], P('dp', 'tp'), parts along dimension 0
- output 4: bfloat16 [65536, 4096], P(('dp', 'tp')), parts along dimension 0
There are 4 independent parts. The reference program is written for one: setup_inputs(seed, part) draws one part's arguments, and reference() takes and returns one part's arrays. A program takes and returns all parts, laid end to end along the dimension named above; an argument that names none is the same for every part.
All inputs are finite; a program needn't handle non-finite values.
Results may differ from the reference program's by a relative error of at most 0.012.
Values are sent between devices in bfloat16 or wider.
A program may use at most 2 GiB of HBM per device.

```python
import jax
import jax.numpy as jnp

ROWS = 2048
D = 4096
FF = 16384


def act(gate, up):
    return jax.nn.silu(gate) * up


def setup_inputs(seed: int = 0, part: int = 0) -> dict:
    kx, ky, ka, kb, kg, ku, kd = jax.random.split(jax.random.key(seed), 7)
    kx, ky, ka, kb = (jax.random.fold_in(k, part) for k in (kx, ky, ka, kb))
    drawn = {
        "x": jax.random.normal(kx, (ROWS, D), jnp.float32),
        "dy": jax.random.normal(ky, (ROWS, D), jnp.float32),
        "gate": jax.random.normal(ka, (ROWS, FF), jnp.float32),
        "up": jax.random.normal(kb, (ROWS, FF), jnp.float32),
        "w_gate": jax.random.normal(kg, (D, FF), jnp.float32) * D**-0.5,
        "w_up": jax.random.normal(ku, (D, FF), jnp.float32) * D**-0.5,
        "w_down": jax.random.normal(kd, (FF, D), jnp.float32) * FF**-0.5,
    }
    return {k: v.astype(jnp.bfloat16) for k, v in drawn.items()}


def reference(x, dy, gate, up, w_gate, w_up, w_down):
    hidden, back = jax.vjp(act, gate.astype(jnp.float32), up.astype(jnp.float32))
    d_hidden = jnp.dot(dy, w_down.T, preferred_element_type=jnp.float32)
    d_gate, d_up = (g.astype(jnp.bfloat16) for g in back(d_hidden))
    dx = jnp.dot(d_gate, w_gate.T, preferred_element_type=jnp.float32) + jnp.dot(d_up, w_up.T, preferred_element_type=jnp.float32)
    dw_gate = jnp.dot(x.T, d_gate, preferred_element_type=jnp.float32)
    dw_up = jnp.dot(x.T, d_up, preferred_element_type=jnp.float32)
    dw_down = jnp.dot(hidden.astype(jnp.bfloat16).T, dy, preferred_element_type=jnp.float32)
    return tuple(g.astype(jnp.bfloat16) for g in (dx, dw_gate, dw_up, dw_down))
```

```python
import jax
import jax.numpy as jnp
from jax import lax
from jax.experimental import pallas as pl
from jax.experimental.pallas import tpu as pltpu
from jax.sharding import PartitionSpec as P

f32, bf = jnp.float32, jnp.bfloat16
NT = (((1,), (1,)), ((), ()))
TN = (((0,), (0,)), ((), ()))
MESH = pl.DeviceIdType.MESH
ANY = pl.BlockSpec(memory_space=pl.ANY)

T, D, F = 2048, 4096, 2048
R = 512
N = 1024
H = R // 2
NP1 = 24
NW = 16
NB = 16
K0 = 5
LAST = NP1 + NW
END = LAST + 3


def ds(start, size):
    return pl.ds(start if isinstance(start, int) else pl.multiple_of(start, size), size)


def copy(a, b, s):
    return pltpu.make_async_copy(a, b, s)


def start(copies):
    for c in copies:
        c.start()


def wait(copies):
    for c in copies:
        c.wait()


def kernel_a(x, dy, gate, up, wg, wu, wd, dgu, hid, dwg, dwu, dx,
             W, dyb, gub, dgb, Pb, Qb, Yb, Ib, Sb,
             semw, semi, semo, semd, r_i, s_i, r_x, s_x, r_y, s_y, r_f, s_fe, s_fm, r_p, s_p, s_l):
    t = lax.axis_index("tp")
    z, core = t // 2, t % 2
    peer = z * 2 + 1 - core
    edge = (z == 0) | (z == 3)
    outer = jnp.where(z < 2, core, 6 + core)
    inner = jnp.where(z < 2, 4 + core, 2 + core)
    mine = jnp.where(z < 2, 0, 1)
    theirs = 1 - mine
    middle = jnp.where(z < 2, 2 + core, 4 + core)

    def remote(a, b, s, r, to):
        return pltpu.make_async_remote_copy(a, b, s, r, device_id={"tp": to}, device_id_type=MESH)

    def loads_a(k, slot):
        i = k % 6
        return [copy(wd.at[ds(i * N, N), :], W.at[slot], semw.at[slot, 0])]

    def loads_b(k, slot):
        j = k % 6 - 2
        return [copy(wg.at[ds(j * N, N), :], W.at[slot, :, pl.ds(0, F)], semw.at[slot, 0]),
                copy(wu.at[ds(j * N, N), :], W.at[slot, :, pl.ds(F, F)], semw.at[slot, 1])]

    def loads_w(k, slot):
        i, j = (k - NP1) // 4, (k - NP1) % 4
        return [copy(x.at[pl.ds(0, N), ds(i * N, N)], W.at[slot, :, pl.ds(0, N)], semw.at[slot, 0]),
                copy(x.at[pl.ds(N, N), ds(i * N, N)], W.at[slot, :, pl.ds(N, N)], semw.at[slot, 1]),
                copy(dgu.at[pl.ds(0, N), ds(j * N, N)], W.at[slot, :, pl.ds(2 * N, N)], semw.at[slot, 2]),
                copy(dgu.at[pl.ds(N, N), ds(j * N, N)], W.at[slot, :, pl.ds(3 * N, N)], semw.at[slot, 3])]

    def in_loads(r):
        return [copy(dy.at[ds(r * R, R), :], dyb, semi.at[0]),
                copy(gate.at[ds(r * R, R), :], gub.at[0], semi.at[1]),
                copy(up.at[ds(r * R, R), :], gub.at[1], semi.at[2])]

    def outs_g(r):
        return [copy(dgb, dgu.at[ds(r * R, R), :], semo.at[0]),
                copy(gub.at[0], hid.at[ds(r * R, R), :], semo.at[1])]

    def outs_w(k, dst):
        slot, i, j = k % 2, (k - NP1) // 4, (k - NP1) % 2
        return [copy(dyb.at[:, ds(slot * 2 * N + h * N, N)],
                     dst.at[ds(i * N + h * R, R), ds(j * N, N)], semd.at[slot, h]) for h in range(2)]

    def kind(k):
        first = k < NP1
        return first & (k % 6 < 2), first & (k % 6 >= 2), jnp.logical_not(first) & (k < LAST)

    start(in_loads(0))
    start(loads_a(0, 0))
    barrier = pltpu.get_barrier_semaphore()
    pl.semaphore_signal(barrier, inc=1, device_id={"tp": peer}, device_id_type=MESH)

    @pl.when(edge)
    def _():
        pl.semaphore_signal(barrier, inc=1, device_id={"tp": middle}, device_id_type=MESH)

    @pl.when(jnp.logical_not(edge))
    def _():
        pl.semaphore_signal(barrier, inc=1, device_id={"tp": outer}, device_id_type=MESH)
        pl.semaphore_signal(barrier, inc=1, device_id={"tp": inner}, device_id_type=MESH)
    pl.semaphore_wait(barrier, jnp.where(edge, 2, 3))

    def region(b, c, h):
        return dx.at[ds((b // 4) * R + c * H, H), ds((b % 4) * N + h * R, R)]

    def pair_send(b):
        s = b % 2
        return remote(Sb.at[s], Ib.at[s], s_i.at[s], r_i.at[s], peer)

    def x_send(b, h):
        return remote(Qb.at[b, h], Qb.at[b, h], s_x.at[h, b], r_x.at[h, b], middle)

    def y_send(b):
        return remote(Qb.at[b, theirs], Yb.at[b], s_y.at[b], r_y.at[b], inner)

    def y_recv(b):
        return remote(Qb.at[b, mine], Yb.at[b], s_y.at[b], r_y.at[b], inner)

    def f_edge(b):
        return remote(Qb.at[b, mine], region(b, core, mine), s_fe.at[mine, b], r_f.at[mine, b], outer)

    def f_inner(b):
        return remote(Qb.at[b, mine], region(b, core, mine), s_fm.at[b], r_f.at[mine, b], inner)

    def f_on(b):
        return remote(region(b, core, theirs), region(b, core, theirs), s_fe.at[theirs, b], r_f.at[theirs, b], outer)

    def f_recv(b, h):
        return remote(region(b, core, h), region(b, core, h), s_fe.at[h, b], r_f.at[h, b], outer)

    def p_own(b):
        return remote(Qb.at[b, mine], region(b, core, mine), s_p.at[mine, b], r_p.at[mine, b], peer)

    def p_on(b, h):
        return remote(region(b, core, h), region(b, core, h), s_p.at[h, b], r_p.at[h, b], peer)

    def p_recv(b, h):
        return remote(region(b, 1 - core, h), region(b, 1 - core, h), s_p.at[h, b], r_p.at[h, b], peer)

    def local(b):
        return copy(Qb.at[b, mine], region(b, core, mine), s_l.at[b])

    def rows(body):
        def go(i, _):
            body(ds(i * 64, 64))
            return 0
        lax.fori_loop(0, H // 64, go, 0)

    def tick(k):
        q = k % 6
        made = (k < NP1) & (q >= 2)
        before = jnp.where(k >= 1, k - 1, 0)
        had = (k >= 1) & (k <= NP1) & (before % 6 >= 2)
        blk = (before // 6) * 4 + before % 6 - 2

        @pl.when(had)
        def _():
            b = blk
            pair_send(b).wait_recv()

            @pl.when(edge)
            def _():
                def add(rs):
                    for h in range(2):
                        Qb[b, h, rs, :] = (Pb[b, h, rs, :] + Ib[b % 2, h, rs, :].astype(f32)).astype(bf)
                rows(add)
                x_send(b, theirs).start()
                x_send(b, mine).start()

            @pl.when(jnp.logical_not(edge))
            def _():
                def add(rs):
                    for h in range(2):
                        Pb[b, h, rs, :] = Pb[b, h, rs, :] + Ib[b % 2, h, rs, :].astype(f32)
                rows(add)

        @pl.when(made)
        def _():
            pair_send((k // 6) * 4 + q - 2).start()

        v = jnp.where(k >= K0, (k - K0) * 4, 0)
        due = (k >= K0) & (v % 9 < 4) & (k < LAST)
        m_main = v // 9
        steady = due
        m = jnp.where(steady, m_main, k - LAST + 16)
        go = steady | (k >= LAST)

        @pl.when(go & jnp.logical_not(edge))
        def _():
            @pl.when(m < NB)
            def _():
                b = m
                x_send(b, theirs).wait_recv()

                def add(rs):
                    Qb[b, theirs, rs, :] = (Pb[b, theirs, rs, :] + Qb[b, theirs, rs, :].astype(f32)).astype(bf)
                rows(add)
                y_send(b).start()

            @pl.when((m >= 1) & (m <= NB))
            def _():
                b = m - 1
                x_send(b, mine).wait_recv()
                y_recv(b).wait_recv()

                def add(rs):
                    Qb[b, mine, rs, :] = (Pb[b, mine, rs, :] + Qb[b, mine, rs, :].astype(f32)
                                          + Yb[b, rs, :].astype(f32)).astype(bf)
                rows(add)
                f_inner(b).start()
                f_edge(b).start()
                p_own(b).start()
                local(b).start()

            @pl.when((m >= 2) & (m <= NB + 1))
            def _():
                b = m - 2
                f_recv(b, theirs).wait_recv()
                f_on(b).start()
                p_on(b, theirs).start()

        @pl.when(go & edge & (m >= 3) & (m <= NB + 2))
        def _():
            b = m - 3
            for h in range(2):
                f_recv(b, h).wait_recv()
                p_on(b, h).start()

    def trip(k, _):
        slot = k % 2
        is_a, is_b, is_w = kind(k)
        next_a, next_b, next_w = kind(k + 1)
        r = k // 6

        @pl.when(is_a)
        def _():
            @pl.when(k % 6 == 0)
            def _():
                wait(in_loads(r))

                @pl.when(r > 0)
                def _():
                    outs_g(r - 1)[0].wait()
            wait(loads_a(k, slot))

        @pl.when(is_b)
        def _():
            wait(loads_b(k, slot))

            @pl.when(k % 6 == 3)
            def _():
                outs_g(r)[1].wait()

                @pl.when(r < 3)
                def _():
                    start(in_loads(r + 1)[1:])

        @pl.when(is_w)
        def _():
            wait(loads_w(k, slot))

        @pl.when(next_a)
        def _():
            start(loads_a(k + 1, 1 - slot))

        @pl.when(next_b)
        def _():
            start(loads_b(k + 1, 1 - slot))

        @pl.when(k == NP1 - 1)
        def _():
            outs_g(3)[0].wait()

        @pl.when(next_w)
        def _():
            start(loads_w(k + 1, 1 - slot))

        @pl.when(is_a)
        def _():
            i = k % 6
            sub = 512
            for n in range(N // sub):
                h = lax.dot_general(dyb[...], W[slot, pl.ds(n * sub, sub), :], NT, preferred_element_type=f32)
                cs, cs2 = ds(i * N + n * sub, sub), ds(F + i * N + n * sub, sub)
                g, u = gub[0, :, cs].astype(f32), gub[1, :, cs].astype(f32)
                sg = jax.nn.sigmoid(g)
                sl = g * sg
                gub[0, :, cs] = (sl * u).astype(bf)
                dgb[:, cs2] = (h * sl).astype(bf)
                dgb[:, cs] = ((h * u) * (sg + sl * (1.0 - sg))).astype(bf)

            @pl.when(i == 1)
            def _():
                start(outs_g(r))

                @pl.when(r < 3)
                def _():
                    in_loads(r + 1)[0].start()

        @pl.when(is_b)
        def _():
            b = r * 4 + k % 6 - 2
            s = b % 2

            @pl.when(b >= 2)
            def _():
                pair_send(b).wait_send()
            d = lax.dot_general(dgb[...], W[slot], NT, preferred_element_type=f32)
            for h in range(2):
                lo, hi = d[:H, h * R:(h + 1) * R], d[H:, h * R:(h + 1) * R]
                Pb[b, h] = jnp.where(core == 0, lo, hi)
                Sb[s, h] = jnp.where(core == 0, hi, lo).astype(bf)

        @pl.when(is_w)
        def _():
            @pl.when(k >= NP1 + 2)
            def _():
                wait(outs_w(k - 2, dwg))
            sub = 512
            for n in range(N // sub):
                s1 = lax.dot_general(W[slot, :, 0:N], W[slot, :, pl.ds(2 * N + n * sub, sub)], TN, preferred_element_type=f32)
                s2 = lax.dot_general(W[slot, :, N:2 * N], W[slot, :, pl.ds(3 * N + n * sub, sub)], TN, preferred_element_type=f32)
                s = (s1 + s2).astype(bf)
                for h in range(2):
                    dyb[:, ds(slot * 2 * N + h * N + n * sub, sub)] = s[h * R:(h + 1) * R]
            j = (k - NP1) % 4

            @pl.when(j < 2)
            def _():
                start(outs_w(k, dwg))

            @pl.when(j >= 2)
            def _():
                start(outs_w(k, dwu))

        tick(k)
        return 0

    lax.fori_loop(0, END, trip, 0)

    for k in (LAST - 2, LAST - 1):
        wait(outs_w(k, dwu))
    for s in range(2):
        pair_send(s).wait_send()

    def finish(b, _):
        for h in range(2):
            p_recv(b, h).wait_recv()
            p_on(b, h).wait_send()

        @pl.when(edge)
        def _():
            for h in range(2):
                x_send(b, h).wait_send()

        @pl.when(jnp.logical_not(edge))
        def _():
            y_send(b).wait_send()
            f_edge(b).wait_send()
            f_inner(b).wait_send()
            f_on(b).wait_send()
            local(b).wait()
        return 0

    lax.fori_loop(0, NB, finish, 0)


def run_a(x, dy, gate, up, wg, wu, wd):
    S = jax.ShapeDtypeStruct
    dma = pltpu.SemaphoreType.DMA
    return pl.pallas_call(
        kernel_a,
        in_specs=[ANY] * 7,
        out_specs=[ANY] * 5,
        out_shape=[S((T, 2 * F), bf), S((T, F), bf), S((D, F), bf), S((D, F), bf), S((T, D), bf)],
        scratch_shapes=[
            pltpu.VMEM((2, N, D), bf), pltpu.VMEM((R, D), bf), pltpu.VMEM((2, R, F), bf),
            pltpu.VMEM((R, 2 * F), bf),
            pltpu.VMEM((NB, 2, H, R), f32), pltpu.VMEM((NB, 2, H, R), bf), pltpu.VMEM((NB, H, R), bf),
            pltpu.VMEM((2, 2, H, R), bf), pltpu.VMEM((2, 2, H, R), bf),
            dma((2, 4)), dma((3,)), dma((2,)), dma((2, 2)),
            dma((2,)), dma((2,)), dma((2, NB)), dma((2, NB)), dma((NB,)), dma((NB,)),
            dma((2, NB)), dma((2, NB)), dma((NB,)), dma((2, NB)), dma((2, NB)), dma((NB,)),
        ],
        compiler_params=pltpu.CompilerParams(vmem_limit_bytes=67043328, collective_id=0, has_side_effects=True),
    )(x, dy, gate, up, wg, wu, wd)


def kernel_c(hid, dy, dxa, dga, dua, out, dx, dg, du, bx, bg, bu, semi, semo):
    s = pl.program_id(0)
    n = pl.num_programs(0)

    def ins(i):
        m = i % 3
        return [copy(dxa.at[ds(i * 256, 256), :], bx.at[m], semi.at[m, 0]),
                copy(dga.at[ds(i * 512, 512), :], bg.at[m], semi.at[m, 1]),
                copy(dua.at[ds(i * 512, 512), :], bu.at[m], semi.at[m, 2])]

    def outs(i):
        m = i % 3
        return [copy(bx.at[m], dx.at[ds(i * 256, 256), :], semo.at[m, 0]),
                copy(bg.at[m], dg.at[ds(i * 512, 512), :], semo.at[m, 1]),
                copy(bu.at[m], du.at[ds(i * 512, 512), :], semo.at[m, 2])]

    @pl.when(s == 0)
    def _():
        start(ins(0))

    @pl.when(s >= 2)
    def _():
        wait(outs(s - 2))

    @pl.when(s + 1 < n)
    def _():
        start(ins(s + 1))
    wait(ins(s))
    start(outs(s))
    out[...] = lax.dot_general(hid[...], dy[...], TN, preferred_element_type=f32).astype(bf)

    @pl.when(s == n - 1)
    def _():
        wait(outs(s - 1))
        wait(outs(s))


def run_c(hid, dy, dxa, dga, dua):
    S = jax.ShapeDtypeStruct
    return pl.pallas_call(
        kernel_c,
        grid=(8,),
        in_specs=[pl.BlockSpec((T, N), lambda s: (0, s // 4)), pl.BlockSpec((T, N), lambda s: (0, s % 4)), ANY, ANY, ANY],
        out_specs=[pl.BlockSpec((N, N), lambda s: (s // 4, s % 4)), ANY, ANY, ANY],
        out_shape=[S((F, D), bf), S((T, D), bf), S((D, F), bf), S((D, F), bf)],
        scratch_shapes=[pltpu.VMEM((3, 256, D), bf), pltpu.VMEM((3, 512, F), bf), pltpu.VMEM((3, 512, F), bf),
                        pltpu.SemaphoreType.DMA((3, 3)), pltpu.SemaphoreType.DMA((3, 3))],
        compiler_params=pltpu.CompilerParams(vmem_limit_bytes=60 * 2**20),
    )(hid, dy, dxa, dga, dua)


def solution(mesh):
    def step(x, dy, gate, up, wg, wu, wd):
        _, hid, dga, dua, dxa = run_a(x, dy, gate, up, wg, wu, wd)
        dwd, dx, dwg, dwu = run_c(hid, dy, dxa, dga, dua)
        return dx, dwg, dwu, dwd

    tokens, columns, rows = P("dp", None), P(None, "tp"), P("tp", None)
    return jax.shard_map(
        step,
        mesh=mesh,
        in_specs=(tokens, tokens, P("dp", "tp"), P("dp", "tp"), columns, columns, rows),
        out_specs=(tokens, P("dp", "tp"), P("dp", "tp"), P(("dp", "tp"), None)),
        check_vma=False,
    )
```

```python
import jax
import jax.numpy as jnp
from jax import lax
from jax.experimental import pallas as pl
from jax.experimental.pallas import tpu as pltpu
from jax.sharding import PartitionSpec as P

f32, bf = jnp.float32, jnp.bfloat16
NT = (((1,), (1,)), ((), ()))
TN = (((0,), (0,)), ((), ()))
MESH = pl.DeviceIdType.MESH
ANY = pl.BlockSpec(memory_space=pl.ANY)

T, D, F = 2048, 4096, 2048
R = 512
N = 1024
H = R // 2
NP1 = 24
NW = 16
NB = 16
K0 = 4
LAST = NP1 + NW
NUM, DEN = 25, 23
LAG = 4
ELAG = 7
FL = 2
Q = H // 2
NP = 2 * NB
TAIL = 2
KEEP = NP - 2 * TAIL


def ds(start, size):
    return pl.ds(start if isinstance(start, int) else pl.multiple_of(start, size), size)


def copy(a, b, s):
    return pltpu.make_async_copy(a, b, s)


def start(copies):
    for c in copies:
        c.start()


def wait(copies):
    for c in copies:
        c.wait()


def kernel_a(x, dy, gate, up, wg, wu, wd, dgu, hid, dwg, dwu, dx, fin,
             W, dyb, gub, dgb, Pb, Qb, Yb, Ib, Sb,
             semw, semi, semo, semd, r_i, s_i, r_x, s_x, r_y, s_y, r_f, s_fe, s_fm, r_p, s_p, s_l, r_pf, s_pf):
    t = lax.axis_index("tp")
    z, core = t // 2, t % 2
    peer = z * 2 + 1 - core
    edge = (z == 0) | (z == 3)
    outer = jnp.where(z < 2, core, 6 + core)
    inner = jnp.where(z < 2, 4 + core, 2 + core)
    mine = jnp.where(z < 2, 0, 1)
    theirs = 1 - mine
    middle = jnp.where(z < 2, 2 + core, 4 + core)

    def remote(a, b, s, r, to):
        return pltpu.make_async_remote_copy(a, b, s, r, device_id={"tp": to}, device_id_type=MESH)

    def loads_a(k, slot):
        i = k % 6
        return [copy(wd.at[ds(i * N, N), :], W.at[slot], semw.at[slot, 0])]

    def loads_b(k, slot):
        j = k % 6 - 2
        return [copy(wg.at[ds(j * N, N), :], W.at[slot, :, pl.ds(0, F)], semw.at[slot, 0]),
                copy(wu.at[ds(j * N, N), :], W.at[slot, :, pl.ds(F, F)], semw.at[slot, 1])]

    def loads_w(k, slot):
        i, j = (k - NP1) // 4, (k - NP1) % 4
        return [copy(x.at[pl.ds(0, N), ds(i * N, N)], W.at[slot, :, pl.ds(0, N)], semw.at[slot, 0]),
                copy(x.at[pl.ds(N, N), ds(i * N, N)], W.at[slot, :, pl.ds(N, N)], semw.at[slot, 1]),
                copy(dgu.at[pl.ds(0, N), ds(j * N, N)], W.at[slot, :, pl.ds(2 * N, N)], semw.at[slot, 2]),
                copy(dgu.at[pl.ds(N, N), ds(j * N, N)], W.at[slot, :, pl.ds(3 * N, N)], semw.at[slot, 3])]

    def part(q, n):
        return pl.ds(q * n, n)

    def loads_dy(r, q, n):
        return [copy(dy.at[ds(r * R + q * n, n), :], dyb.at[part(q, n)], semi.at[0, q])]

    def loads_gate(r, q, n):
        return [copy(gate.at[ds(r * R + q * n, n), :], gub.at[0, part(q, n)], semi.at[1, q])]

    def loads_up(r, q, n):
        return [copy(up.at[ds(r * R + q * n, n), :], gub.at[1, part(q, n)], semi.at[2, q])]

    def loads_gu(r, q, n):
        return loads_gate(r, q, n) + loads_up(r, q, n)

    def outs_g(r, q, n):
        return [copy(dgb.at[part(q, n)], dgu.at[ds(r * R + q * n, n), :], semo.at[0, q])]

    def outs_h(r, q, n):
        return [copy(gub.at[0, part(q, n)], hid.at[ds(r * R + q * n, n), :], semo.at[1, q])]

    def outs_w(k, dst):
        slot, i, j = k % 2, (k - NP1) // 4, (k - NP1) % 2
        return [copy(dyb.at[:, ds(slot * 2 * N + h * N, N)],
                     dst.at[ds(i * N + h * R, R), ds(j * N, N)], semd.at[slot, h]) for h in range(2)]

    start(loads_a(0, 0))
    start(loads_dy(0, 0, R) + loads_gu(0, 0, R))
    barrier = pltpu.get_barrier_semaphore()
    pl.semaphore_signal(barrier, inc=1, device_id={"tp": peer}, device_id_type=MESH)

    @pl.when(edge)
    def _():
        pl.semaphore_signal(barrier, inc=1, device_id={"tp": middle}, device_id_type=MESH)

    @pl.when(jnp.logical_not(edge))
    def _():
        pl.semaphore_signal(barrier, inc=1, device_id={"tp": outer}, device_id_type=MESH)
        pl.semaphore_signal(barrier, inc=1, device_id={"tp": inner}, device_id_type=MESH)
    pl.semaphore_wait(barrier, jnp.where(edge, 2, 3))

    def piece(ref, u, h=None):
        ref = ref.at[u // 2] if h is None else ref.at[u // 2, h]
        return ref.at[ds(u % 2 * Q, Q), :]

    def region(u, c, h):
        b = u // 2
        return dx.at[ds((b // 4) * R + c * H + u % 2 * Q, Q), ds((b % 4) * N + h * R, R)]

    def pair_send(b):
        s = b % 2
        return remote(Sb.at[s], Ib.at[s], s_i.at[s], r_i.at[s], peer)

    def x_send(u, h):
        return remote(piece(Qb, u, h), piece(Qb, u, h), s_x, r_x.at[h, u], middle)

    def y_send(u):
        return remote(piece(Qb, u, theirs), piece(Yb, u), s_y, r_y.at[u], inner)

    def f_edge(u):
        return remote(piece(Qb, u, mine), region(u, core, mine), s_fe, r_f.at[mine, u], outer)

    def f_inner(u):
        return remote(piece(Qb, u, mine), region(u, core, mine), s_fm, r_f.at[mine, u], inner)

    def f_on(u, h):
        a = region(u, core, h)
        return remote(a, a, s_fe, r_f.at[h, u], outer)

    def p_own(u):
        return remote(piece(Qb, u, mine), region(u, core, mine), s_p, r_p, peer)

    def p_on(u, h):
        a = region(u, core, h)
        return remote(a, a, s_p, r_p, peer)

    def fin_at(u, c):
        v = u - KEEP
        return fin.at[v // 2, ds(c * H + v % 2 * Q, Q), :]

    def p_fin(u):
        return remote(piece(Qb, u, mine), fin_at(u, core), s_pf, r_pf, peer)

    def local_fin(u):
        return copy(piece(Qb, u, mine), fin_at(u, core), s_l)

    def local(u):
        return copy(piece(Qb, u, mine), region(u, core, mine), s_l)

    def pair(b):
        pair_send(b).wait_recv()

        @pl.when(edge)
        def _():
            for g in range(2):
                rs = pl.ds(g * Q, Q)
                for h in range(2):
                    Qb[b, h, rs, :] = (Pb[b, h, rs, :] + Ib[b % 2, h, rs, :].astype(f32)).astype(bf)
            for g in range(2):
                x_send(2 * b + g, theirs).start()
                x_send(2 * b + g, mine).start()

        @pl.when(jnp.logical_not(edge))
        def _():
            for g in range(2):
                rs = pl.ds(g * Q, Q)
                for h in range(2):
                    Pb[b, h, rs, :] = Pb[b, h, rs, :] + Ib[b % 2, h, rs, :].astype(f32)

    def pass_on(u):
        b, rs = u // 2, ds(u % 2 * Q, Q)
        x_send(u, theirs).wait_recv()
        Qb[b, theirs, rs, :] = (Pb[b, theirs, rs, :] + Qb[b, theirs, rs, :].astype(f32)).astype(bf)
        y_send(u).start()

    def finish(u):
        b, rs = u // 2, ds(u % 2 * Q, Q)
        x_send(u, mine).wait_recv()
        y_send(u).wait_recv()
        Qb[b, mine, rs, :] = (Pb[b, mine, rs, :] + Qb[b, mine, rs, :].astype(f32) + Yb[b, rs, :].astype(f32)).astype(bf)

        @pl.when(u < KEEP)
        def _():
            f_inner(u).start()
            f_edge(u).start()
            p_own(u).start()
            local(u).start()

        @pl.when(u >= KEEP)
        def _():
            p_fin(u).start()
            local_fin(u).start()

    def hand_on(u):
        f_on(u, theirs).wait_recv()
        f_on(u, theirs).start()
        p_on(u, theirs).start()

    def arrive(u):
        for h in range(2):
            f_on(u, h).wait_recv()
            p_on(u, h).start()

    def tick(k):
        v = jnp.where(k >= K0, (k - K0) * DEN, 0)
        u = v // NUM
        due = (k >= K0) & (v - u * NUM < DEN)

        @pl.when(due & jnp.logical_not(edge))
        def _():
            @pl.when(u < NP)
            def _():
                pass_on(u)

            @pl.when((u >= FL) & (u - FL < NP))
            def _():
                finish(u - FL)

            @pl.when((u >= LAG) & (u - LAG < KEEP))
            def _():
                hand_on(u - LAG)

        @pl.when(due & edge & (u >= ELAG) & (u - ELAG < KEEP))
        def _():
            arrive(u - ELAG)

    def trip_a(r, i):
        slot, k = i, r * 6 + i
        wait(loads_a(k, slot))

        @pl.when(i == 0)
        def _():
            @pl.when(r == 0)
            def _():
                wait(loads_dy(0, 0, R) + loads_gu(0, 0, R))

            @pl.when(r > 0)
            def _():
                for q in range(4):
                    wait(loads_dy(r, q, R // 4) + outs_g(r - 1, q, R // 4))
                for q in range(2):
                    wait(loads_gu(r, q, R // 2))
            start(loads_a(1, 1))

        @pl.when(i == 1)
        def _():
            start(loads_b(2, 0))
        sub = 512
        for n in range(N // sub):
            h = lax.dot_general(dyb[...], W[slot, pl.ds(n * sub, sub), :], NT, preferred_element_type=f32)
            cs, cs2 = ds(i * N + n * sub, sub), ds(F + i * N + n * sub, sub)
            g, u = gub[0, :, cs].astype(f32), gub[1, :, cs].astype(f32)
            sg = jax.nn.sigmoid(g)
            sl = g * sg
            gub[0, :, cs] = (sl * u).astype(bf)
            dgb[:, cs2] = (h * sl).astype(bf)
            dgb[:, cs] = ((h * u) * (sg + sl * (1.0 - sg))).astype(bf)
        @pl.when((i == 0) & (r > 0))
        def _():
            pair(r * 4 - 1)
        tick(k)

    def trip_b(r, j):
        slot, k, b = j % 2, r * 6 + 2 + j, r * 4 + j
        s = b % 2
        wait(loads_b(j + 2, slot))

        @pl.when(j < 3)
        def _():
            start(loads_b(j + 3, 1 - slot))
        for q in range(4):
            @pl.when(j == q)
            def _():
                for o in ((0,), (1,), (2, 3), ())[q]:
                    start(outs_g(r, o, R // 4))
                if q < 2:
                    start(outs_h(r, q, R // 2))

                    @pl.when(r < 3)
                    def _():
                        start(loads_dy(r + 1, q, R // 4) + loads_up(r + 1, q, R // 2))
                else:
                    wait(outs_h(r, q - 2, R // 2))

                    @pl.when(r < 3)
                    def _():
                        start(loads_dy(r + 1, q, R // 4) + loads_gate(r + 1, q - 2, R // 2))
                if q == 3:
                    @pl.when(r < 3)
                    def _():
                        start(loads_a(0, 0))

                    @pl.when(r == 3)
                    def _():
                        for o in range(4):
                            wait(outs_g(3, o, R // 4))
                        start(loads_w(NP1, 0))
        @pl.when(b >= 2)
        def _():
            pair_send(b).wait_send()
        d = lax.dot_general(dgb[...], W[slot], NT, preferred_element_type=f32)
        for h in range(2):
            lo, hi = d[:H, h * R:(h + 1) * R], d[H:, h * R:(h + 1) * R]
            Pb[b, h] = jnp.where(core == 0, lo, hi)
            Sb[s, h] = jnp.where(core == 0, hi, lo).astype(bf)
        @pl.when((j > 0) & (b != 1))
        def _():
            pair(b - 1)
        pair_send(b).start()

        @pl.when(b == 0)
        def _():
            pair(0)
        tick(k)

    def trip_w(t):
        slot, k = t % 2, t + NP1
        wait(loads_w(k, slot))

        @pl.when(t < NW - 1)
        def _():
            start(loads_w(k + 1, 1 - slot))

        @pl.when(t >= 2)
        def _():
            wait(outs_w(k - 2, dwg))
        sub = 512
        for n in range(N // sub):
            s1 = lax.dot_general(W[slot, :, 0:N], W[slot, :, pl.ds(2 * N + n * sub, sub)], TN, preferred_element_type=f32)
            s2 = lax.dot_general(W[slot, :, N:2 * N], W[slot, :, pl.ds(3 * N + n * sub, sub)], TN, preferred_element_type=f32)
            s = (s1 + s2).astype(bf)
            for h in range(2):
                dyb[:, ds(slot * 2 * N + h * N + n * sub, sub)] = s[h * R:(h + 1) * R]
        j = t % 4

        @pl.when(j < 2)
        def _():
            start(outs_w(k, dwg))

        @pl.when(j >= 2)
        def _():
            start(outs_w(k, dwu))
        @pl.when(t == 0)
        def _():
            pair(NB - 1)
        tick(k)

    def each(n, body):
        def go(i, _):
            body(i)
            return 0
        lax.fori_loop(0, n, go, 0)

    def chunk(r):
        each(2, lambda i: trip_a(r, i))
        each(4, lambda j: trip_b(r, j))

    each(4, chunk)
    each(NW, trip_w)

    for k in (LAST - 2, LAST - 1):
        wait(outs_w(k, dwu))

    done = (LAST - 1 - K0) * DEN // NUM

    @pl.when(jnp.logical_not(edge))
    def _():
        for u in range(done + 1, NP + FL):
            if u < NP:
                pass_on(u)
            if u - FL < NP:
                finish(u - FL)
            if u - LAG < KEEP:
                hand_on(u - LAG)

    @pl.when(edge)
    def _():
        for u in range(done - ELAG + 1, KEEP):
            arrive(u)
    for s in range(2):
        pair_send(s).wait_send()

    full, most = pl.ds(0, NB), pl.ds(0, NB - TAIL)

    def all_of(ref, n, s, r):
        return remote(ref.at[n], ref.at[n], s, r, peer)

    both = all_of(Qb, most, s_p, r_p)
    both.wait_recv()
    both.wait_send()

    @pl.when(edge)
    def _():
        all_of(Qb, full, s_x, r_p).wait_send()

    @pl.when(jnp.logical_not(edge))
    def _():
        all_of(Yb, full, s_y, r_p).wait_send()
        all_of(Qb, most, s_fe, r_p).wait_send()
        all_of(Yb, most, s_fm, r_p).wait_send()
        all_of(Yb, pl.ds(0, TAIL), s_pf, r_pf).wait()
        copy(Yb, Yb, s_l).wait()


def run_a(x, dy, gate, up, wg, wu, wd):
    S = jax.ShapeDtypeStruct
    dma = pltpu.SemaphoreType.DMA
    return pl.pallas_call(
        kernel_a,
        in_specs=[ANY] * 7,
        out_specs=[ANY] * 6,
        out_shape=[S((T, 2 * F), bf), S((T, F), bf), S((D, F), bf), S((D, F), bf), S((T, D), bf), S((TAIL, R, R), bf)],
        scratch_shapes=[
            pltpu.VMEM((2, N, D), bf), pltpu.VMEM((R, D), bf), pltpu.VMEM((2, R, F), bf),
            pltpu.VMEM((R, 2 * F), bf),
            pltpu.VMEM((NB, 2, H, R), f32), pltpu.VMEM((NB, 2, H, R), bf), pltpu.VMEM((NB, H, R), bf),
            pltpu.VMEM((2, 2, H, R), bf), pltpu.VMEM((2, 2, H, R), bf),
            dma((2, 4)), dma((3, 4)), dma((2, 4)), dma((2, 2)),
            dma((2,)), dma((2,)), dma((2, NP)), dma(()), dma((NP,)), dma(()),
            dma((2, NP)), dma(()), dma(()), dma(()), dma(()), dma(()), dma(()), dma(()),
        ],
        compiler_params=pltpu.CompilerParams(vmem_limit_bytes=67043328, collective_id=0, has_side_effects=True),
    )(x, dy, gate, up, wg, wu, wd)


SLOTS = 5
STEPS = 8


def kernel_c(hid, dy, dxa, dga, dua, out, dx, dg, du, bx, bg, bu, semi, semo):
    s = pl.program_id(0)
    ahead = 3

    def parts(i, into):
        m = i % SLOTS
        pairs = [(dxa, bx, dx, T // STEPS), (dga, bg, dg, D // STEPS), (dua, bu, du, D // STEPS)]
        if into:
            return [copy(a.at[ds(i * n, n), :], b.at[m], semi.at[m, p]) for p, (a, b, _, n) in enumerate(pairs)]
        return [copy(b.at[m], c.at[ds(i * n, n), :], semo.at[m, p]) for p, (_, b, c, n) in enumerate(pairs)]

    @pl.when(s == 0)
    def _():
        for i in range(ahead):
            start(parts(i, True))

    @pl.when(s >= SLOTS - ahead)
    def _():
        wait(parts(s - SLOTS + ahead, False))

    @pl.when(s + ahead < STEPS)
    def _():
        start(parts(s + ahead, True))
    wait(parts(s, True))
    start(parts(s, False))
    out[...] = lax.dot_general(hid[...], dy[...], TN, preferred_element_type=f32).astype(bf)

    @pl.when(s == STEPS - 1)
    def _():
        for i in range(STEPS - SLOTS + ahead, STEPS):
            wait(parts(i, False))


def run_c(hid, dy, dxa, dga, dua):
    S = jax.ShapeDtypeStruct
    dma = pltpu.SemaphoreType.DMA
    n = D // STEPS
    return pl.pallas_call(
        kernel_c,
        grid=(STEPS,),
        in_specs=[pl.BlockSpec((T, F), lambda s: (0, 0)), pl.BlockSpec((T, n), lambda s: (0, s)), ANY, ANY, ANY],
        out_specs=[pl.BlockSpec((F, n), lambda s: (0, s)), ANY, ANY, ANY],
        out_shape=[S((F, D), bf), S((T, D), bf), S((D, F), bf), S((D, F), bf)],
        scratch_shapes=[pltpu.VMEM((SLOTS, T // STEPS, D), bf), pltpu.VMEM((SLOTS, D // STEPS, F), bf),
                        pltpu.VMEM((SLOTS, D // STEPS, F), bf), dma((SLOTS, 3)), dma((SLOTS, 3))],
        cost_estimate=pl.CostEstimate(flops=2 * T * F * D, bytes_accessed=150 * 2**20, transcendentals=0),
        compiler_params=pltpu.CompilerParams(vmem_limit_bytes=67043328),
    )(hid, dy, dxa, dga, dua)


def kernel_d(dx, fin, near, other, far, out, buf, semi, semo):
    z = lax.axis_index("tp") // 2
    first = D - TAIL * N
    for i in range(4):
        @pl.when(z == i)
        def _():
            for h, a in enumerate(((near, far), (fin, other), (other, fin), (far, near))[i]):
                copy(a, buf.at[h], semi.at[h]).start()
    for h in range(2):
        copy(fin, buf.at[h], semi.at[h]).wait()
        parts = [copy(buf.at[h, b], out.at[pl.ds(T - R, R), pl.ds(first + b * N + h * R, R)], semo.at[h, b]) for b in range(TAIL)]
        start(parts)
    for h in range(2):
        wait([copy(buf.at[h, b], out.at[pl.ds(T - R, R), pl.ds(first + b * N + h * R, R)], semo.at[h, b]) for b in range(TAIL)])


def run_d(dx, *parts):
    dma = pltpu.SemaphoreType.DMA
    return pl.pallas_call(
        kernel_d,
        in_specs=[ANY] * 5,
        out_specs=ANY,
        out_shape=jax.ShapeDtypeStruct((T, D), bf),
        scratch_shapes=[pltpu.VMEM((2, TAIL, R, R), bf), dma((2,)), dma((2, TAIL))],
        input_output_aliases={0: 0},
    )(dx, *parts)


def solution(mesh):
    def step(x, dy, gate, up, wg, wu, wd):
        _, hid, dga, dua, dxa, fin = run_a(x, dy, gate, up, wg, wu, wd)

        def send(to1, to2):
            return lax.ppermute(fin, "tp", [(2 + c, 2 * to1 + c) for c in (0, 1)] + [(4 + c, 2 * to2 + c) for c in (0, 1)])
        near, other, far = send(0, 3), send(2, 1), send(3, 0)
        dwd, dx, dwg, dwu = run_c(hid, dy, dxa, dga, dua)
        dx = run_d(dx, fin, near, other, far)
        return dx, dwg, dwu, dwd

    tokens, columns, rows = P("dp", None), P(None, "tp"), P("tp", None)
    return jax.shard_map(
        step,
        mesh=mesh,
        in_specs=(tokens, tokens, P("dp", "tp"), P("dp", "tp"), columns, columns, rows),
        out_specs=(tokens, P("dp", "tp"), P("dp", "tp"), P(("dp", "tp"), None)),
        check_vma=False,
    )
```

```python
import jax
import jax.numpy as jnp
from jax import lax
from jax.experimental import pallas as pl
from jax.experimental.pallas import tpu as pltpu
from jax.sharding import PartitionSpec as P

f32, bf = jnp.float32, jnp.bfloat16
NT = (((1,), (1,)), ((), ()))
TN = (((0,), (0,)), ((), ()))
MESH = pl.DeviceIdType.MESH
ANY = pl.BlockSpec(memory_space=pl.ANY)

T, D, F = 2048, 4096, 2048
R = 512
N = 1024
H = R // 2
NP1 = 24
NW = 16
NB = 16
K0 = 4
LAST = NP1 + NW
NUM, DEN = 25, 23
LAG = 4
ELAG = 7
FL = 2
Q = H // 2
NP = 2 * NB
TAIL = 2
KEEP = NP - 2 * TAIL


def ds(start, size):
    return pl.ds(start if isinstance(start, int) else pl.multiple_of(start, size), size)


def copy(a, b, s):
    return pltpu.make_async_copy(a, b, s)


def start(copies):
    for c in copies:
        c.start()


def wait(copies):
    for c in copies:
        c.wait()


def kernel_a(x, dy, gate, up, wg, wu, wd, dgu, hid, dwg, dwu, dx, fin,
             W, dyb, gub, dgb, Pb, Qb, Yb, Ib, Sb,
             semw, semi, semo, semd, r_i, s_i, r_x, s_x, r_y, s_y, r_f, s_fe, s_fm, r_p, s_p, s_l, r_pf, s_pf):
    t = lax.axis_index("tp")
    z, core = t // 2, t % 2
    peer = z * 2 + 1 - core
    edge = (z == 0) | (z == 3)
    outer = jnp.where(z < 2, core, 6 + core)
    inner = jnp.where(z < 2, 4 + core, 2 + core)
    mine = jnp.where(z < 2, 0, 1)
    theirs = 1 - mine
    middle = jnp.where(z < 2, 2 + core, 4 + core)

    def remote(a, b, s, r, to):
        return pltpu.make_async_remote_copy(a, b, s, r, device_id={"tp": to}, device_id_type=MESH)

    def loads_a(k, slot):
        i = k % 6
        return [copy(wd.at[ds(i * N, N), :], W.at[slot], semw.at[slot, 0])]

    def loads_b(k, slot):
        j = k % 6 - 2
        return [copy(wg.at[ds(j * N, N), :], W.at[slot, :, pl.ds(0, F)], semw.at[slot, 0]),
                copy(wu.at[ds(j * N, N), :], W.at[slot, :, pl.ds(F, F)], semw.at[slot, 1])]

    def loads_w(k, slot):
        i, j = (k - NP1) // 4, (k - NP1) % 4
        return [copy(x.at[pl.ds(0, N), ds(i * N, N)], W.at[slot, :, pl.ds(0, N)], semw.at[slot, 0]),
                copy(x.at[pl.ds(N, N), ds(i * N, N)], W.at[slot, :, pl.ds(N, N)], semw.at[slot, 1]),
                copy(dgu.at[pl.ds(0, N), ds(j * N, N)], W.at[slot, :, pl.ds(2 * N, N)], semw.at[slot, 2]),
                copy(dgu.at[pl.ds(N, N), ds(j * N, N)], W.at[slot, :, pl.ds(3 * N, N)], semw.at[slot, 3])]

    def part(q, n):
        return pl.ds(q * n, n)

    def loads_dy(r, q, n):
        return [copy(dy.at[ds(r * R + q * n, n), :], dyb.at[part(q, n)], semi.at[0, q])]

    def loads_gate(r, q, n):
        return [copy(gate.at[ds(r * R + q * n, n), :], gub.at[0, part(q, n)], semi.at[1, q])]

    def loads_up(r, q, n):
        return [copy(up.at[ds(r * R + q * n, n), :], gub.at[1, part(q, n)], semi.at[2, q])]

    def loads_gu(r, q, n):
        return loads_gate(r, q, n) + loads_up(r, q, n)

    def first_gu(i):
        return [copy(a.at[pl.ds(0, R), pl.ds(i * N, N)], gub.at[p, :, pl.ds(i * N, N)], semi.at[1 + p, i])
                for p, a in enumerate((gate, up))]

    def outs_g(r, q, n):
        return [copy(dgb.at[part(q, n)], dgu.at[ds(r * R + q * n, n), :], semo.at[0, q])]

    def outs_h(r, q, n):
        return [copy(gub.at[0, part(q, n)], hid.at[ds(r * R + q * n, n), :], semo.at[1, q])]

    def outs_w(k, dst):
        slot, i, j = k % 2, (k - NP1) // 4, (k - NP1) % 2
        return [copy(dyb.at[:, ds(slot * 2 * N + h * N, N)],
                     dst.at[ds(i * N + h * R, R), ds(j * N, N)], semd.at[slot, h]) for h in range(2)]

    start(loads_a(0, 0))
    start(loads_dy(0, 0, R) + first_gu(0) + first_gu(1))
    barrier = pltpu.get_barrier_semaphore()
    pl.semaphore_signal(barrier, inc=1, device_id={"tp": peer}, device_id_type=MESH)

    @pl.when(edge)
    def _():
        pl.semaphore_signal(barrier, inc=1, device_id={"tp": middle}, device_id_type=MESH)

    @pl.when(jnp.logical_not(edge))
    def _():
        pl.semaphore_signal(barrier, inc=1, device_id={"tp": outer}, device_id_type=MESH)
        pl.semaphore_signal(barrier, inc=1, device_id={"tp": inner}, device_id_type=MESH)

    def piece(ref, u, h=None):
        ref = ref.at[u // 2] if h is None else ref.at[u // 2, h]
        return ref.at[ds(u % 2 * Q, Q), :]

    def region(u, c, h):
        b = u // 2
        return dx.at[ds((b // 4) * R + c * H + u % 2 * Q, Q), ds((b % 4) * N + h * R, R)]

    def pair_send(b):
        s = b % 2
        return remote(Sb.at[s], Ib.at[s], s_i.at[s], r_i.at[s], peer)

    def x_send(u, h):
        return remote(piece(Qb, u, h), piece(Qb, u, h), s_x, r_x.at[h, u], middle)

    def y_send(u):
        return remote(piece(Qb, u, theirs), piece(Yb, u), s_y, r_y.at[u], inner)

    def f_edge(u):
        return remote(piece(Qb, u, mine), region(u, core, mine), s_fe, r_f.at[mine, u], outer)

    def f_inner(u):
        return remote(piece(Qb, u, mine), region(u, core, mine), s_fm, r_f.at[mine, u], inner)

    def f_on(u, h):
        a = region(u, core, h)
        return remote(a, a, s_fe, r_f.at[h, u], outer)

    def p_own(u):
        return remote(piece(Qb, u, mine), region(u, core, mine), s_p, r_p, peer)

    def p_on(u, h):
        a = region(u, core, h)
        return remote(a, a, s_p, r_p, peer)

    def fin_at(u, c):
        v = u - KEEP
        return fin.at[v // 2, ds(c * H + v % 2 * Q, Q), :]

    def p_fin(u):
        return remote(piece(Qb, u, mine), fin_at(u, core), s_pf, r_pf, peer)

    def local_fin(u):
        return copy(piece(Qb, u, mine), fin_at(u, core), s_l)

    def local(u):
        return copy(piece(Qb, u, mine), region(u, core, mine), s_l)

    def pair(b):
        pair_send(b).wait_recv()

        @pl.when(edge)
        def _():
            for g in range(2):
                rs = pl.ds(g * Q, Q)
                for h in range(2):
                    Qb[b, h, rs, :] = (Pb[b, h, rs, :] + Ib[b % 2, h, rs, :].astype(f32)).astype(bf)
            for g in range(2):
                x_send(2 * b + g, theirs).start()
                x_send(2 * b + g, mine).start()

        @pl.when(jnp.logical_not(edge))
        def _():
            for g in range(2):
                rs = pl.ds(g * Q, Q)
                for h in range(2):
                    Pb[b, h, rs, :] = Pb[b, h, rs, :] + Ib[b % 2, h, rs, :].astype(f32)

    def pass_on(u):
        b, rs = u // 2, ds(u % 2 * Q, Q)
        x_send(u, theirs).wait_recv()
        Qb[b, theirs, rs, :] = (Pb[b, theirs, rs, :] + Qb[b, theirs, rs, :].astype(f32)).astype(bf)
        y_send(u).start()

    def finish(u):
        b, rs = u // 2, ds(u % 2 * Q, Q)
        x_send(u, mine).wait_recv()
        y_send(u).wait_recv()
        Qb[b, mine, rs, :] = (Pb[b, mine, rs, :] + Qb[b, mine, rs, :].astype(f32) + Yb[b, rs, :].astype(f32)).astype(bf)

        @pl.when(u < KEEP)
        def _():
            f_inner(u).start()
            f_edge(u).start()
            p_own(u).start()
            local(u).start()

        @pl.when(u >= KEEP)
        def _():
            p_fin(u).start()
            local_fin(u).start()

    def hand_on(u):
        f_on(u, theirs).wait_recv()
        f_on(u, theirs).start()
        p_on(u, theirs).start()

    def arrive(u):
        for h in range(2):
            f_on(u, h).wait_recv()
            p_on(u, h).start()

    def tick(k):
        v = jnp.where(k >= K0, (k - K0) * DEN, 0)
        u = v // NUM
        due = (k >= K0) & (v - u * NUM < DEN)

        @pl.when(due & jnp.logical_not(edge))
        def _():
            @pl.when(u < NP)
            def _():
                pass_on(u)

            @pl.when((u >= FL) & (u - FL < NP))
            def _():
                finish(u - FL)

            @pl.when((u >= LAG) & (u - LAG < KEEP))
            def _():
                hand_on(u - LAG)

        @pl.when(due & edge & (u >= ELAG) & (u - ELAG < KEEP))
        def _():
            arrive(u - ELAG)

    def trip_a(r, i):
        slot, k = i, r * 6 + i
        wait(loads_a(k, slot))

        @pl.when(i == 0)
        def _():
            @pl.when(r == 0)
            def _():
                wait(loads_dy(0, 0, R) + first_gu(0))

            @pl.when(r > 0)
            def _():
                for q in range(4):
                    wait(loads_dy(r, q, R // 4) + outs_g(r - 1, q, R // 4))
                for q in range(2):
                    wait(loads_gu(r, q, R // 2))
            start(loads_a(1, 1))

        @pl.when(i == 1)
        def _():
            @pl.when(r == 0)
            def _():
                wait(first_gu(1))
            start(loads_b(2, 0))
        sub = 512
        for n in range(N // sub):
            h = lax.dot_general(dyb[...], W[slot, pl.ds(n * sub, sub), :], NT, preferred_element_type=f32)
            cs, cs2 = ds(i * N + n * sub, sub), ds(F + i * N + n * sub, sub)
            g, u = gub[0, :, cs].astype(f32), gub[1, :, cs].astype(f32)
            sg = jax.nn.sigmoid(g)
            sl = g * sg
            gub[0, :, cs] = (sl * u).astype(bf)
            dgb[:, cs2] = (h * sl).astype(bf)
            dgb[:, cs] = ((h * u) * (sg + sl * (1.0 - sg))).astype(bf)
        @pl.when((i == 1) & (r == 0))
        def _():
            pl.semaphore_wait(barrier, jnp.where(edge, 2, 3))

        @pl.when((i == 0) & (r > 0))
        def _():
            pair(r * 4 - 1)
        tick(k)

    def trip_b(r, j):
        slot, k, b = j % 2, r * 6 + 2 + j, r * 4 + j
        s = b % 2
        wait(loads_b(j + 2, slot))

        @pl.when(j < 3)
        def _():
            start(loads_b(j + 3, 1 - slot))
        for q in range(4):
            @pl.when(j == q)
            def _():
                for o in ((0,), (1,), (2, 3), ())[q]:
                    start(outs_g(r, o, R // 4))
                if q < 2:
                    start(outs_h(r, q, R // 2))

                    @pl.when(r < 3)
                    def _():
                        start(loads_dy(r + 1, q, R // 4) + loads_up(r + 1, q, R // 2))
                else:
                    wait(outs_h(r, q - 2, R // 2))

                    @pl.when(r < 3)
                    def _():
                        start(loads_dy(r + 1, q, R // 4) + loads_gate(r + 1, q - 2, R // 2))
                if q == 3:
                    @pl.when(r < 3)
                    def _():
                        start(loads_a(0, 0))

                    @pl.when(r == 3)
                    def _():
                        for o in range(4):
                            wait(outs_g(3, o, R // 4))
                        start(loads_w(NP1, 0))
        @pl.when(b >= 2)
        def _():
            pair_send(b).wait_send()
        d = lax.dot_general(dgb[...], W[slot], NT, preferred_element_type=f32)
        for h in range(2):
            lo, hi = d[:H, h * R:(h + 1) * R], d[H:, h * R:(h + 1) * R]
            Pb[b, h] = jnp.where(core == 0, lo, hi)
            Sb[s, h] = jnp.where(core == 0, hi, lo).astype(bf)
        @pl.when((j > 0) & (b != 1))
        def _():
            pair(b - 1)
        pair_send(b).start()

        @pl.when(b == 0)
        def _():
            pair(0)
        tick(k)

    def trip_w(t):
        slot, k = t % 2, t + NP1
        wait(loads_w(k, slot))

        @pl.when(t < NW - 1)
        def _():
            start(loads_w(k + 1, 1 - slot))

        @pl.when(t >= 2)
        def _():
            wait(outs_w(k - 2, dwg))
        sub = 512
        for n in range(N // sub):
            s1 = lax.dot_general(W[slot, :, 0:N], W[slot, :, pl.ds(2 * N + n * sub, sub)], TN, preferred_element_type=f32)
            s2 = lax.dot_general(W[slot, :, N:2 * N], W[slot, :, pl.ds(3 * N + n * sub, sub)], TN, preferred_element_type=f32)
            s = (s1 + s2).astype(bf)
            for h in range(2):
                dyb[:, ds(slot * 2 * N + h * N + n * sub, sub)] = s[h * R:(h + 1) * R]
        j = t % 4

        @pl.when(j < 2)
        def _():
            start(outs_w(k, dwg))

        @pl.when(j >= 2)
        def _():
            start(outs_w(k, dwu))
        @pl.when(t == 0)
        def _():
            pair(NB - 1)
        tick(k)

    def each(n, body):
        def go(i, _):
            body(i)
            return 0
        lax.fori_loop(0, n, go, 0)

    def chunk(r):
        each(2, lambda i: trip_a(r, i))
        each(4, lambda j: trip_b(r, j))

    each(4, chunk)
    each(NW, trip_w)

    for k in (LAST - 2, LAST - 1):
        wait(outs_w(k, dwu))

    done = (LAST - 1 - K0) * DEN // NUM

    @pl.when(jnp.logical_not(edge))
    def _():
        for u in range(done + 1, NP + FL):
            if u < NP:
                pass_on(u)
            if u - FL < NP:
                finish(u - FL)
            if u - LAG < KEEP:
                hand_on(u - LAG)

    @pl.when(edge)
    def _():
        for u in range(done - ELAG + 1, KEEP):
            arrive(u)
    for s in range(2):
        pair_send(s).wait_send()

    full, most = pl.ds(0, NB), pl.ds(0, NB - TAIL)

    def all_of(ref, n, s, r):
        return remote(ref.at[n], ref.at[n], s, r, peer)

    both = all_of(Qb, most, s_p, r_p)
    both.wait_recv()
    both.wait_send()

    @pl.when(edge)
    def _():
        all_of(Qb, full, s_x, r_p).wait_send()

    @pl.when(jnp.logical_not(edge))
    def _():
        all_of(Yb, full, s_y, r_p).wait_send()
        all_of(Qb, most, s_fe, r_p).wait_send()
        all_of(Yb, most, s_fm, r_p).wait_send()
        all_of(Yb, pl.ds(0, TAIL), s_pf, r_pf).wait()
        copy(Yb, Yb, s_l).wait()


def run_a(x, dy, gate, up, wg, wu, wd):
    S = jax.ShapeDtypeStruct
    dma = pltpu.SemaphoreType.DMA
    return pl.pallas_call(
        kernel_a,
        in_specs=[ANY] * 7,
        out_specs=[ANY] * 6,
        out_shape=[S((T, 2 * F), bf), S((T, F), bf), S((D, F), bf), S((D, F), bf), S((T, D), bf), S((TAIL, R, R), bf)],
        scratch_shapes=[
            pltpu.VMEM((2, N, D), bf), pltpu.VMEM((R, D), bf), pltpu.VMEM((2, R, F), bf),
            pltpu.VMEM((R, 2 * F), bf),
            pltpu.VMEM((NB, 2, H, R), f32), pltpu.VMEM((NB, 2, H, R), bf), pltpu.VMEM((NB, H, R), bf),
            pltpu.VMEM((2, 2, H, R), bf), pltpu.VMEM((2, 2, H, R), bf),
            dma((2, 4)), dma((3, 4)), dma((2, 4)), dma((2, 2)),
            dma((2,)), dma((2,)), dma((2, NP)), dma(()), dma((NP,)), dma(()),
            dma((2, NP)), dma(()), dma(()), dma(()), dma(()), dma(()), dma(()), dma(()),
        ],
        compiler_params=pltpu.CompilerParams(vmem_limit_bytes=67043328, collective_id=0, has_side_effects=True),
    )(x, dy, gate, up, wg, wu, wd)


SLOTS = 5
STEPS = 8


def kernel_c(hid, dy, dxa, dga, dua, out, dx, dg, du, bx, bg, bu, semi, semo):
    s = pl.program_id(0)
    ahead = 3

    def parts(i, into):
        m = i % SLOTS
        pairs = [(dga, bg, dg, D // STEPS), (dua, bu, du, D // STEPS)]
        n, cut = T // STEPS, D - TAIL * N
        cols = (pl.ds(0, cut), pl.ds(cut, TAIL * N))
        if into:
            return ([copy(a.at[ds(i * n, n), :], b.at[m], semi.at[m, p]) for p, (a, b, _, n) in enumerate(pairs)]
                    + [copy(dxa.at[ds(i * n, n), c], bx.at[m, :, c], semi.at[m, 2 + p]) for p, c in enumerate(cols)])
        return ([copy(b.at[m], c.at[ds(i * n, n), :], semo.at[m, p]) for p, (_, b, c, n) in enumerate(pairs)]
                + [copy(bx.at[m, :, c], dx.at[ds(i * n, n), c], semo.at[m, 2 + p]) for p, c in enumerate(cols)])

    def run(op, i, into):
        copies = parts(i, into)
        op(copies[:-1])

        @pl.when(i < (T - R) // (T // STEPS))
        def _():
            op(copies[-1:])

    @pl.when(s == 0)
    def _():
        for i in range(ahead):
            run(start, i, True)

    @pl.when(s >= SLOTS - ahead)
    def _():
        run(wait, s - SLOTS + ahead, False)

    @pl.when(s + ahead < STEPS)
    def _():
        run(start, s + ahead, True)
    run(wait, s, True)
    run(start, s, False)
    out[...] = lax.dot_general(hid[...], dy[...], TN, preferred_element_type=f32).astype(bf)

    @pl.when(s == STEPS - 1)
    def _():
        for i in range(STEPS - SLOTS + ahead, STEPS):
            run(wait, i, False)


def run_c(hid, dy, dxa, dga, dua):
    S = jax.ShapeDtypeStruct
    dma = pltpu.SemaphoreType.DMA
    n = D // STEPS
    return pl.pallas_call(
        kernel_c,
        grid=(STEPS,),
        in_specs=[pl.BlockSpec((T, F), lambda s: (0, 0)), pl.BlockSpec((T, n), lambda s: (0, s)), ANY, ANY, ANY],
        out_specs=[pl.BlockSpec((F, n), lambda s: (0, s)), ANY, ANY, ANY],
        out_shape=[S((F, D), bf), S((T, D), bf), S((D, F), bf), S((D, F), bf)],
        scratch_shapes=[pltpu.VMEM((SLOTS, T // STEPS, D), bf), pltpu.VMEM((SLOTS, D // STEPS, F), bf),
                        pltpu.VMEM((SLOTS, D // STEPS, F), bf), dma((SLOTS, 4)), dma((SLOTS, 4))],
        cost_estimate=pl.CostEstimate(flops=2 * T * F * D, bytes_accessed=150 * 2**20, transcendentals=0),
        compiler_params=pltpu.CompilerParams(vmem_limit_bytes=67043328),
    )(hid, dy, dxa, dga, dua)


def kernel_d(dx, fin, near, other, far, out, buf, semi, semo):
    z = lax.axis_index("tp") // 2
    first = D - TAIL * N
    for i in range(4):
        @pl.when(z == i)
        def _():
            for h, a in enumerate(((near, far), (fin, other), (other, fin), (far, near))[i]):
                copy(a, buf.at[h], semi.at[h]).start()
    for h in range(2):
        copy(fin, buf.at[h], semi.at[h]).wait()
        parts = [copy(buf.at[h, b], out.at[pl.ds(T - R, R), pl.ds(first + b * N + h * R, R)], semo.at[h, b]) for b in range(TAIL)]
        start(parts)
    for h in range(2):
        wait([copy(buf.at[h, b], out.at[pl.ds(T - R, R), pl.ds(first + b * N + h * R, R)], semo.at[h, b]) for b in range(TAIL)])


def run_d(dx, *parts):
    dma = pltpu.SemaphoreType.DMA
    return pl.pallas_call(
        kernel_d,
        in_specs=[ANY] * 5,
        out_specs=ANY,
        out_shape=jax.ShapeDtypeStruct((T, D), bf),
        scratch_shapes=[pltpu.VMEM((2, TAIL, R, R), bf), dma((2,)), dma((2, TAIL))],
        input_output_aliases={0: 0},
    )(dx, *parts)


def solution(mesh):
    def step(x, dy, gate, up, wg, wu, wd):
        _, hid, dga, dua, dxa, fin = run_a(x, dy, gate, up, wg, wu, wd)

        def send(to1, to2):
            return lax.ppermute(fin, "tp", [(2 + c, 2 * to1 + c) for c in (0, 1)] + [(4 + c, 2 * to2 + c) for c in (0, 1)])
        near, other, far = send(0, 3), send(2, 1), send(3, 0)
        dwd, dx, dwg, dwu = run_c(hid, dy, dxa, dga, dua)
        dx = run_d(dx, fin, near, other, far)
        return dx, dwg, dwu, dwd

    tokens, columns, rows = P("dp", None), P(None, "tp"), P("tp", None)
    return jax.shard_map(
        step,
        mesh=mesh,
        in_specs=(tokens, tokens, P("dp", "tp"), P("dp", "tp"), columns, columns, rows),
        out_specs=(tokens, P("dp", "tp"), P("dp", "tp"), P(("dp", "tp"), None)),
        check_vma=False,
    )
```
